256 devices in a mesh: blk: 64 (over x, z_lo, y, core), pix: 4 (over z_hi).
Axes of the slice: x: 4, y: 4, z: 8 (z_hi: 4, z_lo: 2; z = z_hi * 2 + z_lo), core: 2. Of those that a mesh axis runs over, the one named last changes fastest.
Arguments:
- particles: bfloat16 [32768, 16384], P('blk', 'pix'), may hold values from -10 to 10, as said below
- ctf: bfloat16 [32768, 16384], P('blk', 'pix'), may hold values from -1 to 1
- noise_var: float32 [16384], P('pix'), may hold values from 0.5 to 4
- projections: bfloat16 [1024, 16384], P('blk', 'pix'), may hold values from -3.1 to 3.1
- orient_class: int32 [1024], replicated, may hold values from 0 to 4
- class_prior: float32 [5], replicated, may hold values from -2 to 0
- counts: int32 [64], P('blk'), may hold values from 32 to 512, as said below
Outputs:
- class_field: float32 [1024, 16384], P('blk', 'pix')
- normalizer: float32 [32768], P('blk')
The draws below stay inside these ranges and needn't reach their ends.
Inputs may be any that keep to these rules, and one draw needn't show every extreme that they name: `particles`: real values of particle images. Live slots of each index of blk are its first counts slots; some index of blk is full in every draw.
All inputs are finite; a program needn't handle non-finite values.
Results may differ from the reference program's by a relative error of at most 0.0066.
Values may be sent and summed in bfloat16 or wider, within the bound.
A program may use at most 128 MiB of HBM per device.

```python
import math
import jax
import jax.numpy as jnp
from jax import lax

PIX = 16384
CLASSES = 5
PART_DEV = 512
ORIENTS = 1024
PARTICLES = 32768


def common_fields(key):
    base = jax.random.fold_in(key, 7)
    key_proj, key_ctf, key_noise = jax.random.split(base, 3)
    projection_draw = 0.04 * jax.random.truncated_normal(key_proj, -10.0, 10.0, (ORIENTS, PIX), jnp.float32)
    ctf_draw = jax.random.uniform(key_ctf, (PARTICLES, PIX), jnp.float32, -1.0, 1.0)
    noise_draw = jax.random.truncated_normal(key_noise, -6.0, 6.0, (PARTICLES, PIX), jnp.float32)
    return (projection_draw, ctf_draw, noise_draw)


def draw_particles(key, part):
    return common_fields(key)[2].astype(jnp.bfloat16)


def draw_ctf(key, part):
    return common_fields(key)[1].astype(jnp.bfloat16)


def draw_projections(key, part):
    return common_fields(key)[0].astype(jnp.bfloat16)


def draw_counts(key, part):
    shards = PARTICLES // PART_DEV
    key_level, key_full = jax.random.split(jax.random.fold_in(key, 11))
    level = jax.random.randint(key_level, (shards,), 0, 65)
    full_shard = jax.random.randint(key_full, (), 0, shards)
    level = jnp.where(jnp.arange(shards, dtype=jnp.int32) == full_shard, 64, level)
    lowest = PART_DEV // 16
    return (lowest + (PART_DEV - lowest) * level * level * level // 262144).astype(jnp.int32)


def place_ends(array, key, least, top_value):
    extent = array.shape
    place = [jax.random.randint(jax.random.fold_in(key, axis), (), 0, extent[axis]) for axis in range(len(extent))]
    array = array.at[tuple(place)].set(least)
    longest = extent.index(max(extent))
    place[longest] = (place[longest] + 1) % extent[longest]
    return array.at[tuple(place)].set(top_value)


def block_scale(key, shape, cuts, low, largest):
    def one(dim, parts):
        heights = jax.random.uniform(jax.random.fold_in(jax.random.fold_in(key, 6), dim), (parts,), jnp.float32, low / len(cuts), largest / len(cuts))
        return jnp.repeat(jnp.exp(heights), shape[dim] // parts).reshape((-1,) + (1,) * (len(shape) - dim - 1))

    gain = one(*cuts[0])
    for cut in cuts[1:]:
        gain = gain * one(*cut)
    return gain


def setup_inputs(seed: int = 0) -> dict:
    key_of = jax.random.split(jax.random.key(seed), 8)
    particles = draw_particles(jax.random.fold_in(key_of[7], 71), 0)
    ctf = draw_ctf(jax.random.fold_in(key_of[7], 71), 0)
    noise_var = jnp.clip(jnp.exp(math.log(4.0) - 2.0794415 * jax.random.uniform(key_of[2], (PIX,), jnp.float32) ** block_scale(key_of[2], (PIX,), ((0, 4),), -0.2, 0.2)), 0.5, 4.0)
    projections = draw_projections(jax.random.fold_in(key_of[7], 71), 0)
    orient_class = place_ends(jax.random.randint(key_of[4], (ORIENTS,), 0, CLASSES), jax.random.fold_in(key_of[4], 1), 0, CLASSES - 1).astype(jnp.int32)
    class_prior = jnp.clip(jax.random.uniform(key_of[5], (CLASSES,), jnp.float32, -2.0, 0.0), -2.0, 0.0)
    counts = draw_counts(jax.random.fold_in(key_of[7], 71), 0)
    return dict(particles=particles, ctf=ctf, noise_var=noise_var, projections=projections, orient_class=orient_class, class_prior=class_prior, counts=counts)


def reference(particles, ctf, noise_var, projections, orient_class, class_prior, counts):
    inverse = 1.0 / noise_var
    ctf_wide = ctf.astype(jnp.float32)
    weighted = (particles.astype(jnp.float32) * ctf_wide * inverse[None, :]).astype(jnp.bfloat16)
    quadratic = (0.5 * ctf_wide * ctf_wide * inverse[None, :]).astype(jnp.bfloat16)
    proj_wide = projections.astype(jnp.float32)
    square = (proj_wide * proj_wide).astype(jnp.bfloat16)
    cross_term = lax.dot_general(weighted, projections, (((1,), (1,)), ((), ())), preferred_element_type=jnp.float32)
    square_term = lax.dot_general(quadratic, square, (((1,), (1,)), ((), ())), preferred_element_type=jnp.float32)
    scores = cross_term - square_term
    member = orient_class[:, None] == jnp.arange(CLASSES, dtype=jnp.int32)[None, :]
    orient_prior = jnp.sum(jnp.where(member, class_prior[None, :], jnp.float32(0.0)), axis=1)
    logits = scores + orient_prior[None, :]
    peak_score = jnp.max(logits, axis=1)
    log_total = peak_score + jnp.log(jnp.sum(jnp.exp(logits - peak_score[:, None]), axis=1))
    slot_index = jnp.arange(PARTICLES, dtype=jnp.int32) % PART_DEV
    shard_index = jnp.arange(PARTICLES, dtype=jnp.int32) // PART_DEV
    live_slot = slot_index < counts[shard_index]
    normalizer = jnp.where(live_slot, log_total, jnp.float32(0.0))
    weights = jnp.where(live_slot[:, None], jnp.exp(logits - log_total[:, None]), jnp.float32(0.0)).astype(jnp.bfloat16)
    class_field = lax.dot_general(weights, weighted, (((0,), (0,)), ((), ())), preferred_element_type=jnp.float32)
    return class_field, normalizer
```

```python
import jax
import jax.numpy as jnp
from jax import lax
from jax.experimental import pallas as pl
from jax.experimental.pallas import tpu as pltpu
from jax.sharding import Mesh
from jax.sharding import PartitionSpec as P

CLASSES = 5
BLK = ("blk_0", "blk_1", "blk_2", "blk_3")
MESH = pl.DeviceIdType.MESH
F32 = jnp.float32
BF16 = jnp.bfloat16
NSEM = 160


def kernel(
    part_hbm, ctf_hbm, nv_ref, own_ref, oc_ref, cp_ref, cnt_ref,
    out_ref, norm_ref,
    wgt, quad, proj, sq, pscore, rq, logit, stats, wts,
    cown, cpart, drecv, fsend, frecv, sbuf, ssend, srecv, zsend, zrecv,
    load_sem, send_sem, agr_sem, rq_sem, st_sem, w_sem, d_sem, f_sem, s_sem, z_sem,
):
    x = lax.axis_index("blk_0")
    z = lax.axis_index("blk_1")
    y = lax.axis_index("blk_2")
    c = lax.axis_index("blk_3")
    q = lax.axis_index("pix")
    npart, npix = part_hbm.shape

    def shifted(a, b):
        nx = lax.rem(x + a * (1 - c) + b * c, 4)
        ny = lax.rem(y + a * c + b * (1 - c), 4)
        return (nx, z, ny, c, q)

    fp, fm, sp, sm = shifted(1, 0), shifted(3, 0), shifted(0, 1), shifted(0, 3)
    zn = (x, 1 - z, y, c, q)
    pn = (x, z, y, 1 - c, q)
    qp, qm, q2 = ((x, z, y, c, lax.rem(q + k, 4)) for k in (1, 3, 2))
    peers = (fp, fm, sp, sm, zn, pn, qp, qm, q2)

    sends = []

    def send(src, dst, rsem, dev):
        copy = pltpu.make_async_remote_copy(
            src_ref=src, dst_ref=dst, send_sem=send_sem.at[len(sends)], recv_sem=rsem,
            device_id=dev, device_id_type=MESH,
        )
        copy.start()
        sends.append(copy)

    def arrived(dst, rsem):
        pltpu.make_async_remote_copy(
            src_ref=dst, dst_ref=dst, send_sem=send_sem.at[0], recv_sem=rsem,
            device_id=pn, device_id_type=MESH,
        ).wait_recv()

    pieces = 4
    rows = npart // pieces
    loads = []
    for i in range(pieces):
        for k, (src, dst) in enumerate(((part_hbm, wgt), (ctf_hbm, quad))):
            cp = pltpu.make_async_copy(
                src.at[pl.ds(i * rows, rows)], dst.at[pl.ds(i * rows, rows)], load_sem.at[2 * i + k]
            )
            cp.start()
            loads.append(cp)

    barrier = pltpu.get_barrier_semaphore()
    for dev in peers:
        pl.semaphore_signal(barrier, inc=1, device_id=dev, device_id_type=MESH)
    pl.semaphore_wait(barrier, len(peers))

    def slab_no(f, s, k, dz):
        return (((f % 4) * 4 + s % 4) * 2 + k) * 2 + dz

    def slab(f, s, k, dz):
        return proj.at[pl.ds(slab_no(f, s, k, dz) * 16, 16)]

    def ag(src, f, s, k, dz, dev):
        send(src, slab(f, s, k, dz), agr_sem.at[slab_no(f, s, k, dz)], dev)

    def ag_wait(f, s, k, dz):
        arrived(slab(f, s, k, dz), agr_sem.at[slab_no(f, s, k, dz)])

    def to_partner(f, s, dz):
        ag(slab(f, s, 0, dz), f, s, 1, dz, pn)

    def to_second(f, dz):
        ag(slab(f, 0, 0, dz), f, 3, 0, dz, sp)
        ag(slab(f, 0, 0, dz), f, 1, 0, dz, sm)

    ag(own_ref, 0, 0, 0, 1, zn)
    ag(own_ref, 3, 0, 0, 0, fp)
    ag(own_ref, 1, 0, 0, 0, fm)
    ag(own_ref, 0, 3, 0, 0, sp)
    ag(own_ref, 0, 1, 0, 0, sm)
    ag(own_ref, 0, 0, 1, 0, pn)
    slab(0, 0, 0, 0)[...] = own_ref[...]

    inverse = 1.0 / nv_ref[...]

    def prepare(i):
        loads[2 * i].wait()
        loads[2 * i + 1].wait()

        @pl.loop(0, rows // 16)
        def _(r):
            at = pl.ds(pl.multiple_of(i * rows + r * 16, 16), 16)
            for h in range(npix // 1024):
                cols = pl.ds(h * 1024, 1024)
                inv = inverse[:, h * 1024 : (h + 1) * 1024]
                wide = quad[at, cols].astype(F32)
                wgt[at, cols] = (wgt[at, cols].astype(F32) * wide * inv).astype(BF16)
                quad[at, cols] = (0.5 * wide * wide * inv).astype(BF16)

    prepare(0)
    prepare(1)
    ag_wait(3, 0, 0, 0)
    ag(slab(3, 0, 0, 0), 2, 0, 0, 0, fp)
    to_partner(3, 0, 0)
    ag_wait(1, 0, 0, 0)
    to_partner(1, 0, 0)
    ag_wait(0, 3, 0, 0)
    ag(slab(0, 3, 0, 0), 0, 2, 0, 0, sp)
    to_partner(0, 3, 0)
    ag_wait(0, 1, 0, 0)
    to_partner(0, 1, 0)
    ag_wait(0, 0, 0, 1)
    ag(slab(0, 0, 0, 1), 3, 0, 0, 1, fp)
    ag(slab(0, 0, 0, 1), 1, 0, 0, 1, fm)
    to_second(0, 1)
    to_second(3, 0)
    to_second(1, 0)
    to_partner(0, 0, 1)
    prepare(2)
    prepare(3)
    ag_wait(0, 3, 0, 1)
    to_partner(0, 3, 1)
    ag_wait(0, 1, 0, 1)
    ag(slab(0, 1, 0, 1), 0, 2, 0, 1, sm)
    to_partner(0, 1, 1)
    ag_wait(1, 0, 0, 1)
    ag(slab(1, 0, 0, 1), 2, 0, 0, 1, fm)
    to_second(1, 1)
    to_partner(1, 0, 1)
    ag_wait(3, 0, 0, 1)
    to_second(3, 1)
    to_partner(3, 0, 1)
    ag_wait(2, 0, 0, 0)
    to_second(2, 0)
    to_partner(2, 0, 0)
    for dz in (0, 1):
        ag_wait(0, 2, 0, dz)
        to_partner(0, 2, dz)

    lane = lax.broadcasted_iota(jnp.int32, (1, 1024), 1)
    prior_row = jnp.zeros((1, 1024), F32)
    for k in range(CLASSES):
        prior_row = jnp.where(oc_ref[...] == k, cp_ref[k], prior_row)
    row = lax.broadcasted_iota(jnp.int32, (256, 1), 0)
    rf, rk, rz, rr = row // 64, (row // 32) % 2, (row // 16) % 2, row % 16
    co = (c + rk) % 2
    ox = (x + rf * (1 - co) + q * co) % 4
    oy = (y + rf * co + q * (1 - co)) % 4
    oz = (z + rz) % 2
    number = (((ox * 2 + oz) * 4 + oy) * 2 + co) * 16 + rr
    prior = jnp.sum(jnp.where(number == lane, prior_row, 0.0), axis=1, keepdims=True)

    nt = (((1,), (1,)), ((), ()))

    def scores(f):
        group = proj.at[pl.ds(f * 256, 256)]

        @pl.loop(0, 16)
        def _(r):
            at = pl.ds(pl.multiple_of(r * 16, 16), 16)
            wide = group[at, :].astype(F32)
            sq[at, :] = (wide * wide).astype(BF16)

        for h in range(npart // 256):
            some = pl.ds(h * 256, 256)
            cross = lax.dot_general(group[...], wgt[some, :], nt, preferred_element_type=F32)
            square = lax.dot_general(sq[...], quad[some, :], nt, preferred_element_type=F32)
            pscore[pl.ds(f * 256, 256), some] = cross - square

    def prow(f, k, half):
        return pl.ds(pl.multiple_of(f * 256 + lax.rem(q + k, 4) * 64 + half * 32, 32), 32)

    def rq_send(f, k, half, slot, dev):
        send(pscore.at[prow(f, k, half)], rq.at[f * 6 + slot], rq_sem.at[f * 6 + slot], dev)

    def rq_wait(f, slot):
        arrived(rq.at[f * 6 + slot], rq_sem.at[f * 6 + slot])

    def rq_first(f):
        rq_send(f, 2, 0, 0, qp)
        rq_send(f, 2, 1, 1, qm)
        rq_send(f, 1, 1, 2, qp)
        rq_send(f, 3, 0, 3, qm)

    def rq_second(f):
        rq_wait(f, 0)
        pscore[prow(f, 1, 0), :] += rq[f * 6]
        rq_send(f, 1, 0, 4, qp)
        rq_wait(f, 1)
        pscore[prow(f, 3, 1), :] += rq[f * 6 + 1]
        rq_send(f, 3, 1, 5, qm)

    def rq_third(f):
        for slot in (2, 3, 4, 5):
            rq_wait(f, slot)
        logit[pl.ds(f * 64, 32), :] = (
            pscore[prow(f, 0, 0), :] + rq[f * 6 + 3] + rq[f * 6 + 4] + prior[f * 64 : f * 64 + 32]
        )
        logit[pl.ds(f * 64 + 32, 32), :] = (
            pscore[prow(f, 0, 1), :] + rq[f * 6 + 2] + rq[f * 6 + 5] + prior[f * 64 + 32 : f * 64 + 64]
        )

    def rest_of_group(f):
        for dz in (0, 1):
            if f == 2 and dz == 1:
                ag_wait(2, 0, 0, 1)
                to_second(2, 1)
                to_partner(2, 0, 1)
            ag_wait(f, 3, 0, dz)
            if dz == 0:
                ag(slab(f, 3, 0, 0), f, 2, 0, 0, sp)
            to_partner(f, 3, dz)
            ag_wait(f, 1, 0, dz)
            if dz == 1:
                ag(slab(f, 1, 0, 1), f, 2, 0, 1, sm)
            to_partner(f, 1, dz)

    def end_of_group(f):
        for dz in (0, 1):
            ag_wait(f, 2, 0, dz)
            to_partner(f, 2, dz)

    def partners_group(f):
        for s in range(4):
            for dz in (0, 1):
                ag_wait(f, s, 1, dz)

    partners_group(0)
    scores(0)
    rq_first(0)
    ag_wait(2, 0, 0, 1)
    to_second(2, 1)
    to_partner(2, 0, 1)

    def group(f):
        for dz in (0, 1):
            ag_wait(f, 3, 0, dz)
            if dz == 0:
                ag(slab(f, 3, 0, 0), f, 2, 0, 0, sp)
            to_partner(f, 3, dz)
            ag_wait(f, 1, 0, dz)
            if dz == 1:
                ag(slab(f, 1, 0, 1), f, 2, 0, 1, sm)
            to_partner(f, 1, dz)
        end_of_group(f)
        partners_group(f)

    order = (0, 1, 3, 2)
    for before, f in zip(order, order[1:]):
        group(f)
        scores(f)
        rq_first(f)
        rq_second(before)
    for f in order[:-1]:
        rq_third(f)
    rq_second(2)
    rq_third(2)

    peak = jnp.max(logit[...], axis=0, keepdims=True)
    total = jnp.sum(jnp.exp(logit[...] - peak), axis=0, keepdims=True)
    stats[0, 0:1, :] = peak
    stats[0, 1:2, :] = total
    for k, dev in ((3, qp), (1, qm), (2, q2)):
        send(stats.at[0], stats.at[k], st_sem.at[k], dev)
    for k in (1, 3, 2):
        arrived(stats.at[k], st_sem.at[k])
    top = peak
    for k in (1, 2, 3):
        top = jnp.maximum(top, stats[k, 0:1, :])
    full = total * jnp.exp(peak - top)
    for k in (1, 2, 3):
        full += stats[k, 1:2, :] * jnp.exp(stats[k, 0:1, :] - top)
    lse = top + jnp.log(full)
    live = lax.broadcasted_iota(jnp.int32, (1, npart), 1) < cnt_ref[0]
    norm_ref[...] = jnp.where(live, lse, 0.0)
    wts[0] = jnp.where(live, jnp.exp(logit[...] - lse), 0.0).astype(BF16)

    def w_half(k, half):
        return wts.at[k, pl.ds(half * 128, 128)]

    def w_send(a, b, half, dev):
        send(w_half(a, half), w_half(b, half), w_sem.at[b * 2 + half], dev)

    def w_wait(k, half):
        arrived(w_half(k, half), w_sem.at[k * 2 + half])

    w_send(0, 3, 0, qp)
    w_send(0, 1, 1, qm)
    w_send(0, 3, 1, qp)
    w_send(0, 1, 0, qm)

    def classes(k):
        @pl.loop(0, npix // 512)
        def _(h):
            cols = pl.ds(pl.multiple_of(h * 512, 512), 512)
            res = jnp.dot(wts[k], wgt[:, cols], preferred_element_type=F32)
            for f in range(4):
                cown[k, pl.ds(f * 32, 32), cols] = res[f * 64 : f * 64 + 32]
                cpart[k, pl.ds(f * 32, 32), cols] = res[f * 64 + 32 : f * 64 + 64].astype(BF16)

        send(cpart.at[k], drecv.at[k], d_sem.at[k], pn)

    def add_partner(k):
        arrived(drecv.at[k], d_sem.at[k])

        @pl.loop(0, npix // 512)
        def _(h):
            cols = pl.ds(pl.multiple_of(h * 512, 512), 512)
            cown[k, :, cols] += drecv[k, :, cols].astype(F32)

    def ring_first(src, out, inc, sem, dp, dm):
        for n, (j, dz, dev) in enumerate(((2, 0, dp), (2, 1, dm), (1, 1, dp), (3, 0, dm))):
            out[n] = src(j, dz)[...].astype(BF16)
            send(out.at[n], inc.at[n], sem.at[n], dev)

    def ring_second(src, out, inc, sem, dp, dm):
        for n, (j, dz, dev) in enumerate(((1, 0, dp), (3, 1, dm))):
            arrived(inc.at[n], sem.at[n])
            out[4 + n] = (src(j, dz)[...] + inc[n].astype(F32)).astype(BF16)
            send(out.at[4 + n], inc.at[4 + n], sem.at[4 + n], dev)

    def ring_third(src, inc, sem):
        for n in (2, 3, 4, 5):
            arrived(inc.at[n], sem.at[n])
        first = src(0, 0)[...] + inc[3].astype(F32) + inc[4].astype(F32)
        second = src(0, 1)[...] + inc[2].astype(F32) + inc[5].astype(F32)
        return first, second

    def f_args(k):
        return (
            lambda j, dz: cown.at[k, pl.ds(j * 32 + dz * 16, 16)],
            fsend.at[pl.ds(k * 6, 6)], frecv.at[pl.ds(k * 6, 6)], f_sem.at[pl.ds(k * 6, 6)], fp, fm,
        )

    def f_third(k):
        src, _, inc, sem, _, _ = f_args(k)
        first, second = ring_third(src, inc, sem)
        at = lax.rem(q + k, 4)
        sbuf[at, 0] = first
        sbuf[at, 1] = second

    classes(0)
    w_wait(3, 0)
    w_send(3, 2, 0, qp)
    w_wait(1, 1)
    w_send(1, 2, 1, qm)
    add_partner(0)
    ring_first(*f_args(0))
    w_wait(3, 1)
    classes(3)
    ring_second(*f_args(0))
    w_wait(1, 0)
    classes(1)
    add_partner(3)
    ring_first(*f_args(3))
    f_third(0)
    add_partner(1)
    ring_first(*f_args(1))
    ring_second(*f_args(3))
    w_wait(2, 0)
    w_wait(2, 1)
    classes(2)
    ring_second(*f_args(1))
    f_third(3)
    add_partner(2)
    ring_first(*f_args(2))
    f_third(1)
    ring_second(*f_args(2))
    f_third(2)

    s_args = (lambda j, dz: sbuf.at[j, dz], ssend, srecv, s_sem, sp, sm)
    ring_first(*s_args)
    ring_second(*s_args)
    mine, other = ring_third(s_args[0], srecv, s_sem)
    zsend[...] = other.astype(BF16)
    send(zsend, zrecv, z_sem, zn)
    out_ref[...] = mine
    arrived(zrecv, z_sem)
    out_ref[...] += zrecv[...].astype(F32)

    for copy in sends:
        copy.wait_send()


def body(particles, ctf, noise_var, projections, orient_class, class_prior, counts):
    npart, npix = particles.shape
    vmem = pl.BlockSpec(memory_space=pltpu.VMEM)
    smem = pl.BlockSpec(memory_space=pltpu.SMEM)
    hbm = pl.BlockSpec(memory_space=pl.ANY)
    dma = pltpu.SemaphoreType.DMA
    out, norm = pl.pallas_call(
        kernel,
        out_shape=(jax.ShapeDtypeStruct((16, npix), F32), jax.ShapeDtypeStruct((1, npart), F32)),
        in_specs=[hbm, hbm, vmem, vmem, vmem, smem, smem],
        out_specs=(vmem, vmem),
        scratch_shapes=[
            pltpu.VMEM((npart, npix), BF16),
            pltpu.VMEM((npart, npix), BF16),
            pltpu.VMEM((1024, npix), BF16),
            pltpu.VMEM((256, npix), BF16),
            pltpu.VMEM((1024, npart), F32),
            pltpu.VMEM((24, 32, npart), F32),
            pltpu.VMEM((256, npart), F32),
            pltpu.VMEM((4, 8, npart), F32),
            pltpu.VMEM((4, 256, npart), BF16),
            pltpu.VMEM((4, 128, npix), F32),
            pltpu.VMEM((4, 128, npix), BF16),
            pltpu.VMEM((4, 128, npix), BF16),
            pltpu.VMEM((24, 16, npix), BF16),
            pltpu.VMEM((24, 16, npix), BF16),
            pltpu.VMEM((4, 2, 16, npix), F32),
            pltpu.VMEM((6, 16, npix), BF16),
            pltpu.VMEM((6, 16, npix), BF16),
            pltpu.VMEM((16, npix), BF16),
            pltpu.VMEM((16, npix), BF16),
            dma((8,)), dma((NSEM,)), dma((64,)), dma((24,)), dma((4,)), dma((8,)), dma((4,)),
            dma((24,)), dma((6,)), dma,
        ],
        compiler_params=pltpu.CompilerParams(
            collective_id=0, has_side_effects=True, vmem_limit_bytes=64 * 1024 * 1024 - 128 * 1024
        ),
    )(particles, ctf, noise_var.reshape(1, npix), projections, orient_class.reshape(1, 1024), class_prior, counts)
    return out, norm.reshape(npart)


def solution(mesh):
    torus = Mesh(
        mesh.devices.reshape(4, 2, 4, 2, mesh.shape["pix"]),
        ("blk_0", "blk_1", "blk_2", "blk_3", "pix"),
    )
    in_specs = (P(BLK, "pix"), P(BLK, "pix"), P("pix"), P(BLK, "pix"), P(), P(), P(BLK))
    out_specs = (P(BLK, "pix"), P(BLK))
    return jax.shard_map(body, mesh=torus, in_specs=in_specs, out_specs=out_specs, check_vma=False)
```

```python
import jax
import jax.numpy as jnp
from jax import lax
from jax.experimental import pallas as pl
from jax.experimental.pallas import tpu as pltpu
from jax.sharding import Mesh
from jax.sharding import PartitionSpec as P

CLASSES = 5
BLK = ("blk_0", "blk_1", "blk_2", "blk_3")
MESH = pl.DeviceIdType.MESH
F32 = jnp.float32
BF16 = jnp.bfloat16
NSEM = 320
CHUNKS = (1, 2, 2, 1)
MAXCH = 4
PLACE = (3, 1, 0, 2)


def kernel(
    part_hbm, ctf_hbm, nv_hbm, own_hbm, oc_hbm, cp_ref, cnt_ref,
    out_ref, norm_ref,
    nv_ref, own_ref, oc_ref,
    wgt, ctf, wgt_t, quad_t, proj, sq, pscore, rq, logit, stats, wts,
    cown, cpart, drecv, fsend, frecv, ssend, srecv, szrecv, szown, zsend, zrecv, wn, scale,
    load_sem, send_sem, agr_sem, rq_sem, st_sem, w_sem, d_sem, f_sem, ss_sem, s_sem, sz_sem, z_sem,
):
    x = lax.axis_index("blk_0")
    z = lax.axis_index("blk_1")
    y = lax.axis_index("blk_2")
    c = lax.axis_index("blk_3")
    q = lax.axis_index("pix")
    npart, npix = part_hbm.shape

    def shifted(a, b):
        nx = lax.rem(x + a * (1 - c) + b * c, 4)
        ny = lax.rem(y + a * c + b * (1 - c), 4)
        return (nx, z, ny, c, q)

    fp, fm, sp, sm = shifted(1, 0), shifted(3, 0), shifted(0, 1), shifted(0, 3)
    zn = (x, 1 - z, y, c, q)
    pn = (x, z, y, 1 - c, q)
    qp, qm, q2 = ((x, z, y, c, lax.rem(q + k, 4)) for k in (1, 3, 2))
    far = [shifted(0, k) for k in (1, 2, 3)]
    peers = (fp, fm, sp, sm, zn, pn, qp, qm, q2, far[1], *((a, 1 - b, *rest) for a, b, *rest in far))

    sends = []

    def send(src, dst, rsem, dev):
        copy = pltpu.make_async_remote_copy(
            src_ref=src, dst_ref=dst, send_sem=send_sem.at[len(sends)], recv_sem=rsem,
            device_id=dev, device_id_type=MESH,
        )
        copy.start()
        sends.append(copy)

    def arrived(dst, rsem):
        pltpu.make_async_remote_copy(
            src_ref=dst, dst_ref=dst, send_sem=send_sem.at[0], recv_sem=rsem,
            device_id=pn, device_id_type=MESH,
        ).wait_recv()

    barrier = pltpu.get_barrier_semaphore()
    for dev in peers:
        pl.semaphore_signal(barrier, inc=1, device_id=dev, device_id_type=MESH)

    small = []
    for i, (src, dst) in enumerate(((own_hbm, own_ref), (nv_hbm, nv_ref), (oc_hbm, oc_ref))):
        cp = pltpu.make_async_copy(src, dst, load_sem.at[8 + i])
        cp.start()
        small.append(cp)
    pieces = 4
    rows = npart // pieces
    loads = []
    for i in range(pieces):
        for k, (src, dst) in enumerate(((part_hbm, wgt), (ctf_hbm, ctf))):
            cp = pltpu.make_async_copy(
                src.at[pl.ds(i * rows, rows)], dst.at[pl.ds(i * rows, rows)], load_sem.at[2 * i + k]
            )
            cp.start()
            loads.append(cp)

    small[0].wait()
    pl.semaphore_wait(barrier, len(peers))

    def slab_no(f, s, k, dz):
        return (((f % 4) * 2 + dz) * 4 + s % 4) * 2 + k

    def slab(f, s, k, dz):
        return proj.at[pl.ds(slab_no(f, s, k, dz) * 16, 16)]

    def ag(src, f, s, k, dz, dev):
        send(src, slab(f, s, k, dz), agr_sem.at[slab_no(f, s, k, dz)], dev)

    def ag_wait(f, s, k, dz):
        arrived(slab(f, s, k, dz), agr_sem.at[slab_no(f, s, k, dz)])

    def to_partner(f, s, dz):
        ag(slab(f, s, 0, dz), f, s, 1, dz, pn)

    def to_second(f, dz):
        ag(slab(f, 0, 0, dz), f, 3, 0, dz, sp)
        ag(slab(f, 0, 0, dz), f, 1, 0, dz, sm)

    ag(own_ref, 0, 0, 0, 1, zn)
    ag(own_ref, 1, 0, 0, 0, fm)
    ag(own_ref, 0, 3, 0, 0, sp)
    slab(0, 0, 0, 0)[...] = own_ref[...]

    small[1].wait()
    small[2].wait()
    def prepare(i):
        loads[2 * i].wait()
        loads[2 * i + 1].wait()
        at = pl.ds(i * rows, rows)

        @pl.loop(0, npix // 256)
        def _(h):
            cols = pl.ds(pl.multiple_of(h * 256, 256), 256)
            inv = 1.0 / nv_ref[:, cols]
            wide = ctf[at, cols].astype(F32)
            weighted = (wgt[at, cols].astype(F32) * wide * inv).astype(BF16)
            wgt[at, cols] = weighted
            wgt_t[cols, at] = weighted.T
            quad_t[cols, at] = (0.5 * wide * wide * inv).astype(BF16).T

    lane = lax.broadcasted_iota(jnp.int32, (1, 1024), 1)
    prior_row = jnp.zeros((1, 1024), F32)
    for k in range(CLASSES):
        prior_row = jnp.where(oc_ref[...] == k, cp_ref[k], prior_row)
    row = lax.broadcasted_iota(jnp.int32, (256, 1), 0)
    rp, rz, rk, rr = row // 64, (row // 32) % 2, (row // 16) % 2, row % 16
    rf = jnp.where(rp == 0, 2, jnp.where(rp == 1, 1, jnp.where(rp == 2, 3, 0)))
    co = (c + rk) % 2
    ox = (x + rf * (1 - co) + q * co) % 4
    oy = (y + rf * co + q * (1 - co)) % 4
    oz = (z + rz) % 2
    number = (((ox * 2 + oz) * 4 + oy) * 2 + co) * 16 + rr
    prior = jnp.sum(jnp.where(number == lane, prior_row, 0.0), axis=1, keepdims=True)

    def scores(g):
        group = proj.at[pl.ds(g * 128, 128)]
        wide = group[...].astype(F32)
        sq[...] = (wide * wide).astype(BF16)
        for h in range(npart // 256):
            some = pl.ds(h * 256, 256)
            cross = jnp.dot(group[...], wgt_t[:, some], preferred_element_type=F32)
            square = jnp.dot(sq[...], quad_t[:, some], preferred_element_type=F32)
            pscore[pl.ds(g * 128, 128), some] = cross - square

    def prow(g, k, half):
        return pl.ds(pl.multiple_of(g * 128 + lax.rem(q + k, 4) * 32 + half * 16, 16), 16)

    def rq_send(g, k, half, slot, dev):
        send(pscore.at[prow(g, k, half)], rq.at[g * 6 + slot], rq_sem.at[g * 6 + slot], dev)

    def rq_wait(g, slot):
        arrived(rq.at[g * 6 + slot], rq_sem.at[g * 6 + slot])

    def rq_far(g):
        rq_send(g, 2, 0, 0, qp)
        rq_send(g, 2, 1, 1, qm)

    def rq_near(g):
        rq_send(g, 1, 1, 2, qp)
        rq_send(g, 3, 0, 3, qm)

    def rq_second(g, way):
        rq_wait(g, way)
        at = prow(g, 1 + 2 * way, way)
        pscore[at, :] += rq[g * 6 + way]
        rq_send(g, 1 + 2 * way, way, 4 + way, (qp, qm)[way])

    def rq_third(g):
        for slot in (2, 3, 4, 5):
            rq_wait(g, slot)
        at = (PLACE[g // 2] * 2 + g % 2) * 32
        logit[pl.ds(at, 16), :] = (
            pscore[prow(g, 0, 0), :] + rq[g * 6 + 3] + rq[g * 6 + 4] + prior[at : at + 16]
        )
        logit[pl.ds(at + 16, 16), :] = (
            pscore[prow(g, 0, 1), :] + rq[g * 6 + 2] + rq[g * 6 + 5] + prior[at + 16 : at + 32]
        )

    def got(f, s, dz):
        ag_wait(f, s, 0, dz)
        if s == 3 and dz == 0:
            ag(slab(f, 3, 0, 0), f, 2, 0, 0, sp)
        if s == 1 and dz == 1:
            ag(slab(f, 1, 0, 1), f, 2, 0, 1, sm)
        if s == 0 and f == 3 and dz == 0:
            ag(slab(3, 0, 0, 0), 2, 0, 0, 0, fp)
        if s == 0 and f == 1 and dz == 1:
            ag(slab(1, 0, 0, 1), 2, 0, 0, 1, fm)
        to_partner(f, s, dz)

    def partners(f, dz):
        for s in range(4):
            ag_wait(f, s, 1, dz)

    live = lax.broadcasted_iota(jnp.int32, (1, npart), 1) < cnt_ref[0]

    def peak():
        most = jnp.max(logit[...], axis=0, keepdims=True)
        e = jnp.exp(logit[...] - most)
        stats[0, 0:1, :] = most
        stats[0, 1:2, :] = jnp.sum(e, axis=0, keepdims=True)
        wts[0] = e.astype(BF16)
        for k, dev in ((3, qp), (1, qm), (2, q2)):
            send(stats.at[0], stats.at[k], st_sem.at[k], dev)

    def softmax():
        for k in (1, 3, 2):
            arrived(stats.at[k], st_sem.at[k])
        peaks = [stats[k, 0:1, :] for k in range(4)]
        top = jnp.maximum(jnp.maximum(peaks[0], peaks[1]), jnp.maximum(peaks[2], peaks[3]))
        full = sum(stats[k, 1:2, :] * jnp.exp(peaks[k] - top) for k in range(4))
        lse = top + jnp.log(full)
        norm_ref[...] = jnp.where(live, lse, 0.0)
        for k in (1, 2, 3):
            scale[k, 0:1, :] = jnp.where(live, jnp.exp(peaks[k] - lse), 0.0)
        wn[0] = jnp.where(live, jnp.exp(logit[...] - lse), 0.0).astype(BF16)

    def w_piece(k, p):
        return wts.at[k, pl.ds(p * 64, 64)]

    def w_send(a, b, p, dev):
        send(w_piece(a, p), w_piece(b, p), w_sem.at[b * 4 + p], dev)

    def w_wait(k, p):
        arrived(w_piece(k, p), w_sem.at[k * 4 + p])
        if k == 3 and p % 2 == 0:
            w_send(3, 2, p, qp)
        if k == 1 and p % 2 == 1:
            w_send(1, 2, p, qm)

    def w_start():
        for p in range(4):
            w_send(0, 3, p, qp)
            w_send(0, 1, p, qm)

    def cols_of(h, n):
        return pl.ds(h * (npix // n), npix // n)

    def classes(k, part, h):
        n = CHUNKS[k]
        base = part * 64
        half = pl.ds(part * 128, 128)
        if k > 0 and h == 0:
            wn[k, half] = (wts[k, half].astype(F32) * scale[k, 0:1, :]).astype(BF16)
        for i in range(npix // n // 512):
            cols = pl.ds(h * (npix // n) + i * 512, 512)
            res = jnp.dot(wn[k, half], wgt[:, cols], preferred_element_type=F32)
            for g in range(4):
                cown[k, pl.ds(base + g * 16, 16), cols] = res[g * 32 : g * 32 + 16]
                cpart[k, pl.ds(base + g * 16, 16), cols] = res[g * 32 + 16 : g * 32 + 32].astype(BF16)
        at = (k, pl.ds(base, 64), cols_of(h, n))
        send(cpart.at[at], drecv.at[at], d_sem.at[(k * 2 + part) * MAXCH + h], pn)

    def own(k, j, dz, cols):
        return cown.at[k, pl.ds((PLACE[j] * 2 + dz) * 16, 16), cols]

    def ring_send(k, h, n, slot, value, dev):
        at = (k * 6 + slot, slice(None), cols_of(h, n))
        fsend[at] = value.astype(BF16)
        send(fsend.at[at], frecv.at[at], f_sem.at[(k * 6 + slot) * MAXCH + h], dev)

    def ring_wait(k, h, n, slot):
        at = (k * 6 + slot, slice(None), cols_of(h, n))
        arrived(frecv.at[at], f_sem.at[(k * 6 + slot) * MAXCH + h])
        return frecv[at].astype(F32)

    def first(k, part, h):
        n = CHUNKS[k]
        at = (k, pl.ds(part * 64, 64), cols_of(h, n))
        arrived(drecv.at[at], d_sem.at[(k * 2 + part) * MAXCH + h])

        def both(j, dz):
            there = drecv[k, pl.ds((PLACE[j] * 2 + dz) * 16, 16), cols_of(h, n)]
            return own(k, j, dz, cols_of(h, n))[...] + there.astype(F32)

        if part == 0:
            ring_send(k, h, n, 0, both(2, 0), fp)
            ring_send(k, h, n, 1, both(2, 1), fm)
            ring_send(k, h, n, 2, both(1, 1), fp)
            rest = ((1, 0),)
        else:
            ring_send(k, h, n, 3, both(3, 0), fm)
            rest = ((3, 1), (0, 0), (0, 1))
        for j, dz in rest:
            own(k, j, dz, cols_of(h, n))[...] = both(j, dz)

    def second(k, h, way):
        n = CHUNKS[k]
        j, dz, dev = ((1, 0, fp), (3, 1, fm))[way]
        value = own(k, j, dz, cols_of(h, n))[...] + ring_wait(k, h, n, way)
        ring_send(k, h, n, 4 + way, value, dev)

    late = []

    def s_wait(k, h):
        at = (k, slice(None) if k != 2 else 0, slice(None), cols_of(h, CHUNKS[k]))

        @pl.when(lax.rem(q + k, 4) != 0)
        def _():
            arrived(srecv.at[at], s_sem.at[k * MAXCH + h])

    def third(k, h):
        n = CHUNKS[k]
        cols = cols_of(h, n)
        parts = [ring_wait(k, h, n, slot) for slot in (2, 3, 4, 5)]
        one = (own(k, 0, 0, cols)[...] + parts[1] + parts[2]).astype(BF16)
        two = (own(k, 0, 1, cols)[...] + parts[0] + parts[3]).astype(BF16)
        s = lax.rem(q + k, 4)
        there = shifted(0, s)
        ssend[k, 0, :, cols] = one
        ssend[k, 1, :, cols] = two
        if k == 2:
            at = (slice(None), cols)
            send(ssend.at[(2, 1, *at)], szrecv.at[at], sz_sem.at[h], (there[0], 1 - z, *there[2:]))
        at = (k, slice(None) if k != 2 else 0, slice(None), cols)
        copy = pltpu.make_async_remote_copy(
            src_ref=ssend.at[at], dst_ref=srecv.at[at],
            send_sem=ss_sem.at[k * MAXCH + h], recv_sem=s_sem.at[k * MAXCH + h],
            device_id=there, device_id_type=MESH,
        )

        @pl.when(s != 0)
        def _():
            copy.start()

        @pl.when(s == 0)
        def _():
            srecv[k, 0, :, cols] = one
            if k != 2:
                srecv[k, 1, :, cols] = two

        late.append((s, copy))

    def zearly():
        for k in (0, 3, 1):
            for h in range(CHUNKS[k]):
                s_wait(k, h)
        for i in range(4):
            cols = cols_of(i, 4)
            mine, other = (
                sum(srecv[k, dz, :, cols].astype(F32) for k in (0, 3, 1)) for dz in (0, 1)
            )
            szown[:, cols] = mine
            zsend[:, cols] = other.astype(BF16)
        send(zsend, zrecv, z_sem, zn)

    def zwait():
        arrived(zrecv, z_sem)

    def final(h):
        cols = cols_of(h, CHUNKS[2])
        at = (slice(None), cols)
        s_wait(2, h)
        arrived(szrecv.at[at], sz_sem.at[h])
        out_ref[at] = (
            szown[at] + zrecv[at].astype(F32) + srecv[2, 0, :, cols].astype(F32) + szrecv[at].astype(F32)
        )

    prepare(3)
    ag(own_ref, 0, 1, 0, 0, sm)
    ag(own_ref, 3, 0, 0, 0, fp)
    prepare(1)
    got(1, 0, 0)
    to_second(1, 0)
    got(0, 1, 0)
    got(0, 0, 1)
    got(0, 3, 0)
    to_second(0, 1)
    prepare(2)
    ag(own_ref, 0, 0, 1, 0, pn)
    got(1, 3, 0)
    ag(slab(0, 0, 0, 1), 1, 0, 0, 1, fm)
    got(0, 2, 0)
    got(0, 1, 1)
    prepare(0)
    got(3, 0, 0)
    partners(0, 0)
    scores(0)
    rq_far(0)
    ag(slab(0, 0, 0, 1), 3, 0, 0, 1, fp)
    rq_near(0)
    to_second(3, 0)
    got(1, 1, 0)
    got(0, 3, 1)
    got(1, 0, 1)
    got(0, 2, 1)
    got(1, 2, 0)
    partners(0, 1)
    to_second(1, 1)
    scores(1)
    rq_far(1)
    partners(1, 0)
    scores(2)
    rq_far(2)
    got(2, 0, 0)
    rq_near(2)
    got(3, 3, 0)
    to_second(2, 0)
    rq_second(0, 0)
    got(2, 0, 1)
    got(1, 1, 1)
    to_second(2, 1)
    got(3, 1, 0)
    rq_second(0, 1)
    got(3, 2, 0)
    got(3, 0, 1)
    rq_near(1)
    rq_second(1, 1)
    rq_second(1, 0)
    rq_second(2, 1)
    got(1, 2, 1)
    to_second(3, 1)
    partners(3, 0)
    scores(6)
    got(2, 3, 0)
    rq_second(2, 0)
    got(2, 1, 1)
    got(2, 3, 1)
    got(1, 3, 1)
    rq_far(6)
    rq_near(6)
    partners(1, 1)
    got(2, 1, 0)
    scores(3)
    got(3, 3, 1)
    rq_far(3)
    got(3, 1, 1)
    rq_third(0)
    got(2, 2, 1)
    partners(2, 1)
    scores(5)
    got(2, 2, 0)
    rq_near(3)
    got(3, 2, 1)
    partners(3, 1)
    partners(2, 0)
    rq_far(5)
    scores(7)
    rq_second(6, 1)
    rq_far(7)
    rq_near(5)
    rq_second(6, 0)
    rq_second(5, 1)
    scores(4)
    rq_second(5, 0)
    rq_far(4)
    rq_third(1)
    rq_second(7, 1)
    rq_near(7)
    rq_third(6)
    rq_near(4)
    rq_second(4, 0)
    rq_third(2)
    rq_second(4, 1)
    rq_second(3, 1)
    rq_second(7, 0)
    rq_second(3, 0)
    rq_third(7)
    rq_third(5)
    rq_third(4)
    rq_third(3)
    peak()
    w_start()
    softmax()
    classes(0, 0, 0)
    classes(0, 1, 0)
    first(0, 0, 0)
    w_wait(3, 1)
    first(0, 1, 0)
    w_wait(1, 0)
    w_wait(1, 1)
    w_wait(3, 0)
    classes(3, 0, 0)
    classes(1, 0, 0)
    second(0, 0, 0)
    classes(1, 0, 1)
    w_wait(1, 2)
    second(0, 0, 1)
    first(3, 0, 0)
    first(1, 0, 0)
    w_wait(3, 3)
    w_wait(3, 2)
    classes(3, 1, 0)
    w_wait(1, 3)
    classes(1, 1, 0)
    first(1, 0, 1)
    classes(1, 1, 1)
    first(3, 1, 0)
    second(3, 0, 1)
    w_wait(2, 1)
    w_wait(2, 0)
    second(3, 0, 0)
    classes(2, 0, 0)
    classes(2, 0, 1)
    first(1, 1, 1)
    second(1, 1, 0)
    third(0, 0)
    second(1, 1, 1)
    second(1, 0, 0)
    first(2, 0, 0)
    first(1, 1, 0)
    w_wait(2, 3)
    w_wait(2, 2)
    classes(2, 1, 0)
    third(3, 0)
    second(1, 0, 1)
    third(1, 1)
    classes(2, 1, 1)
    first(2, 0, 1)
    second(2, 0, 0)
    first(2, 1, 0)
    second(2, 0, 1)
    third(1, 0)
    first(2, 1, 1)
    second(2, 1, 1)
    second(2, 1, 0)
    zearly()
    third(2, 0)
    third(2, 1)
    zwait()
    final(0)
    final(1)

    for s, copy in late:

        @pl.when(s != 0)
        def _():
            copy.wait_send()

    for copy in sends:
        copy.wait_send()


def body(particles, ctf, noise_var, projections, orient_class, class_prior, counts):
    npart, npix = particles.shape
    vmem = pl.BlockSpec(memory_space=pltpu.VMEM)
    smem = pl.BlockSpec(memory_space=pltpu.SMEM)
    hbm = pl.BlockSpec(memory_space=pl.ANY)
    dma = pltpu.SemaphoreType.DMA
    out, norm = pl.pallas_call(
        kernel,
        out_shape=(jax.ShapeDtypeStruct((16, npix), F32), jax.ShapeDtypeStruct((1, npart), F32)),
        in_specs=[hbm, hbm, hbm, hbm, hbm, smem, smem],
        out_specs=(vmem, vmem),
        scratch_shapes=[
            pltpu.VMEM((1, npix), F32),
            pltpu.VMEM((16, npix), BF16),
            pltpu.VMEM((1, 1024), jnp.int32),
            pltpu.VMEM((npart, npix), BF16),
            pltpu.VMEM((npart, npix), BF16),
            pltpu.VMEM((npix, npart), BF16),
            pltpu.VMEM((npix, npart), BF16),
            pltpu.VMEM((1024, npix), BF16),
            pltpu.VMEM((128, npix), BF16),
            pltpu.VMEM((1024, npart), F32),
            pltpu.VMEM((48, 16, npart), F32),
            pltpu.VMEM((256, npart), F32),
            pltpu.VMEM((4, 8, npart), F32),
            pltpu.VMEM((4, 256, npart), BF16),
            pltpu.VMEM((4, 128, npix), F32),
            pltpu.VMEM((4, 128, npix), BF16),
            pltpu.VMEM((4, 128, npix), BF16),
            pltpu.VMEM((24, 16, npix), BF16),
            pltpu.VMEM((24, 16, npix), BF16),
            pltpu.VMEM((4, 2, 16, npix), BF16),
            pltpu.VMEM((4, 2, 16, npix), BF16),
            pltpu.VMEM((16, npix), BF16),
            pltpu.VMEM((16, npix), F32),
            pltpu.VMEM((16, npix), BF16),
            pltpu.VMEM((16, npix), BF16),
            pltpu.VMEM((4, 256, npart), BF16),
            pltpu.VMEM((4, 8, npart), F32),
            dma((11,)), dma((NSEM,)), dma((64,)), dma((48,)), dma((4,)), dma((16,)), dma((8 * MAXCH,)),
            dma((24 * MAXCH,)), dma((4 * MAXCH,)), dma((4 * MAXCH,)), dma((MAXCH,)), dma,
        ],
        compiler_params=pltpu.CompilerParams(
            collective_id=0, has_side_effects=True, vmem_limit_bytes=64 * 1024 * 1024 - 128 * 1024
        ),
    )(particles, ctf, noise_var.reshape(1, npix), projections, orient_class.reshape(1, 1024), class_prior, counts)
    return out, norm.reshape(npart)


def solution(mesh):
    torus = Mesh(
        mesh.devices.reshape(4, 2, 4, 2, mesh.shape["pix"]),
        ("blk_0", "blk_1", "blk_2", "blk_3", "pix"),
    )
    in_specs = (P(BLK, "pix"), P(BLK, "pix"), P("pix"), P(BLK, "pix"), P(), P(), P(BLK))
    out_specs = (P(BLK, "pix"), P(BLK))
    return jax.shard_map(body, mesh=torus, in_specs=in_specs, out_specs=out_specs, check_vma=False)
```

```python
import jax
import jax.numpy as jnp
from jax import lax
from jax.experimental import pallas as pl
from jax.experimental.pallas import tpu as pltpu
from jax.sharding import Mesh
from jax.sharding import PartitionSpec as P

CLASSES = 5
BLK = ("blk_0", "blk_1", "blk_2", "blk_3")
MESH = pl.DeviceIdType.MESH
F32 = jnp.float32
BF16 = jnp.bfloat16
NSEM = 320
CHUNKS = (1, 2, 2, 1)
MAXCH = 4
PLACE = (3, 1, 0, 2)


def kernel(
    part_hbm, ctf_hbm, nv_hbm, own_hbm, oc_hbm, cp_ref, cnt_ref,
    out_ref, norm_ref,
    nv_ref, own_ref, oc_ref,
    wgt, ctf, wgt_t, quad_t, proj, sq, pscore, rq, logit, stats, wts,
    cown, cpart, drecv, fsend, frecv, ssend, srecv, szrecv, szown, zsend, zrecv, wn, scale,
    load_sem, send_sem, agr_sem, rq_sem, st_sem, w_sem, d_sem, f_sem, ss_sem, s_sem, sz_sem, z_sem,
):
    x = lax.axis_index("blk_0")
    z = lax.axis_index("blk_1")
    y = lax.axis_index("blk_2")
    c = lax.axis_index("blk_3")
    q = lax.axis_index("pix")
    npart, npix = part_hbm.shape

    def shifted(a, b):
        nx = lax.rem(x + a * (1 - c) + b * c, 4)
        ny = lax.rem(y + a * c + b * (1 - c), 4)
        return (nx, z, ny, c, q)

    fp, fm, sp, sm = shifted(1, 0), shifted(3, 0), shifted(0, 1), shifted(0, 3)
    zn = (x, 1 - z, y, c, q)
    pn = (x, z, y, 1 - c, q)
    qp, qm, q2 = ((x, z, y, c, lax.rem(q + k, 4)) for k in (1, 3, 2))
    far = [shifted(0, k) for k in (1, 2, 3)]
    peers = (fp, fm, sp, sm, zn, pn, qp, qm, q2, far[1], *((a, 1 - b, *rest) for a, b, *rest in far))

    sends = []

    def send(src, dst, rsem, dev):
        copy = pltpu.make_async_remote_copy(
            src_ref=src, dst_ref=dst, send_sem=send_sem.at[len(sends)], recv_sem=rsem,
            device_id=dev, device_id_type=MESH,
        )
        copy.start()
        sends.append(copy)

    def arrived(dst, rsem):
        pltpu.make_async_remote_copy(
            src_ref=dst, dst_ref=dst, send_sem=send_sem.at[0], recv_sem=rsem,
            device_id=pn, device_id_type=MESH,
        ).wait_recv()

    barrier = pltpu.get_barrier_semaphore()
    for dev in peers:
        pl.semaphore_signal(barrier, inc=1, device_id=dev, device_id_type=MESH)

    small = []
    for i, (src, dst) in enumerate(((own_hbm, own_ref), (nv_hbm, nv_ref), (oc_hbm, oc_ref))):
        cp = pltpu.make_async_copy(src, dst, load_sem.at[8 + i])
        cp.start()
        small.append(cp)
    pieces = 4
    rows = npart // pieces
    loads = []
    for i in range(pieces):
        for k, (src, dst) in enumerate(((part_hbm, wgt), (ctf_hbm, ctf))):
            cp = pltpu.make_async_copy(
                src.at[pl.ds(i * rows, rows)], dst.at[pl.ds(i * rows, rows)], load_sem.at[2 * i + k]
            )
            cp.start()
            loads.append(cp)

    def slab_no(f, s, k, dz):
        return (((f % 4) * 2 + dz) * 4 + s % 4) * 2 + k

    def slab(f, s, k, dz):
        return proj.at[pl.ds(slab_no(f, s, k, dz) * 16, 16)]

    def ag(src, f, s, k, dz, dev):
        send(src, slab(f, s, k, dz), agr_sem.at[slab_no(f, s, k, dz)], dev)

    def ag_wait(f, s, k, dz):
        arrived(slab(f, s, k, dz), agr_sem.at[slab_no(f, s, k, dz)])

    def to_partner(f, s, dz):
        ag(slab(f, s, 0, dz), f, s, 1, dz, pn)

    def to_second(f, dz):
        ag(slab(f, 0, 0, dz), f, 3, 0, dz, sp)
        ag(slab(f, 0, 0, dz), f, 1, 0, dz, sm)

    small[1].wait()
    small[2].wait()

    def prepare(i):
        loads[2 * i].wait()
        loads[2 * i + 1].wait()
        at = pl.ds(i * rows, rows)

        @pl.loop(0, npix // 256)
        def _(h):
            cols = pl.ds(pl.multiple_of(h * 256, 256), 256)
            inv = 1.0 / nv_ref[:, cols]
            wide = ctf[at, cols].astype(F32)
            weighted = (wgt[at, cols].astype(F32) * wide * inv).astype(BF16)
            wgt[at, cols] = weighted
            wgt_t[cols, at] = weighted.T
            quad_t[cols, at] = (0.5 * wide * wide * inv).astype(BF16).T

    prepare(0)
    small[0].wait()
    pl.semaphore_wait(barrier, len(peers))

    ag(own_ref, 0, 0, 0, 1, zn)
    ag(own_ref, 1, 0, 0, 0, fm)
    ag(own_ref, 0, 3, 0, 0, sp)
    slab(0, 0, 0, 0)[...] = own_ref[...]

    lane = lax.broadcasted_iota(jnp.int32, (1, 1024), 1)
    prior_row = jnp.zeros((1, 1024), F32)
    for k in range(CLASSES):
        prior_row = jnp.where(oc_ref[...] == k, cp_ref[k], prior_row)
    row = lax.broadcasted_iota(jnp.int32, (256, 1), 0)
    rp, rz, rk, rr = row // 64, (row // 32) % 2, (row // 16) % 2, row % 16
    rf = jnp.where(rp == 0, 2, jnp.where(rp == 1, 1, jnp.where(rp == 2, 3, 0)))
    co = (c + rk) % 2
    ox = (x + rf * (1 - co) + q * co) % 4
    oy = (y + rf * co + q * (1 - co)) % 4
    oz = (z + rz) % 2
    number = (((ox * 2 + oz) * 4 + oy) * 2 + co) * 16 + rr
    prior = jnp.sum(jnp.where(number == lane, prior_row, 0.0), axis=1, keepdims=True)

    def scores(g):
        group = proj.at[pl.ds(g * 128, 128)]
        wide = group[...].astype(F32)
        sq[...] = (wide * wide).astype(BF16)
        for h in range(npart // 256):
            some = pl.ds(h * 256, 256)
            cross = jnp.dot(group[...], wgt_t[:, some], preferred_element_type=F32)
            square = jnp.dot(sq[...], quad_t[:, some], preferred_element_type=F32)
            pscore[pl.ds(g * 128, 128), some] = cross - square

    def prow(g, k, half):
        return pl.ds(pl.multiple_of(g * 128 + lax.rem(q + k, 4) * 32 + half * 16, 16), 16)

    def rq_send(g, k, half, slot, dev):
        send(pscore.at[prow(g, k, half)], rq.at[g * 6 + slot], rq_sem.at[g * 6 + slot], dev)

    def rq_wait(g, slot):
        arrived(rq.at[g * 6 + slot], rq_sem.at[g * 6 + slot])

    def rq_far(g):
        rq_send(g, 2, 0, 0, qp)
        rq_send(g, 2, 1, 1, qm)

    def rq_near(g):
        rq_send(g, 1, 1, 2, qp)
        rq_send(g, 3, 0, 3, qm)

    def rq_second(g, way):
        rq_wait(g, way)
        at = prow(g, 1 + 2 * way, way)
        pscore[at, :] += rq[g * 6 + way]
        rq_send(g, 1 + 2 * way, way, 4 + way, (qp, qm)[way])

    def rq_third(g):
        for slot in (2, 3, 4, 5):
            rq_wait(g, slot)
        at = (PLACE[g // 2] * 2 + g % 2) * 32
        logit[pl.ds(at, 16), :] = (
            pscore[prow(g, 0, 0), :] + rq[g * 6 + 3] + rq[g * 6 + 4] + prior[at : at + 16]
        )
        logit[pl.ds(at + 16, 16), :] = (
            pscore[prow(g, 0, 1), :] + rq[g * 6 + 2] + rq[g * 6 + 5] + prior[at + 16 : at + 32]
        )

    def got(f, s, dz):
        ag_wait(f, s, 0, dz)
        if s == 3 and dz == 0:
            ag(slab(f, 3, 0, 0), f, 2, 0, 0, sp)
        if s == 1 and dz == 1:
            ag(slab(f, 1, 0, 1), f, 2, 0, 1, sm)
        if s == 0 and f == 3 and dz == 0:
            ag(slab(3, 0, 0, 0), 2, 0, 0, 0, fp)
        if s == 0 and f == 1 and dz == 1:
            ag(slab(1, 0, 0, 1), 2, 0, 0, 1, fm)
        to_partner(f, s, dz)

    def partners(f, dz):
        for s in range(4):
            ag_wait(f, s, 1, dz)

    live = lax.broadcasted_iota(jnp.int32, (1, npart), 1) < cnt_ref[0]

    def peak():
        most = jnp.max(logit[...], axis=0, keepdims=True)
        e = jnp.exp(logit[...] - most)
        stats[0, 0:1, :] = most
        stats[0, 1:2, :] = jnp.sum(e, axis=0, keepdims=True)
        wts[0] = e.astype(BF16)
        for k, dev in ((3, qp), (1, qm), (2, q2)):
            send(stats.at[0], stats.at[k], st_sem.at[k], dev)

    def softmax():
        for k in (1, 3, 2):
            arrived(stats.at[k], st_sem.at[k])
        peaks = [stats[k, 0:1, :] for k in range(4)]
        top = jnp.maximum(jnp.maximum(peaks[0], peaks[1]), jnp.maximum(peaks[2], peaks[3]))
        full = sum(stats[k, 1:2, :] * jnp.exp(peaks[k] - top) for k in range(4))
        lse = top + jnp.log(full)
        norm_ref[...] = jnp.where(live, lse, 0.0)
        for k in (1, 2, 3):
            scale[k, 0:1, :] = jnp.where(live, jnp.exp(peaks[k] - lse), 0.0)
        wn[0] = jnp.where(live, jnp.exp(logit[...] - lse), 0.0).astype(BF16)

    def w_piece(k, p):
        return wts.at[k, pl.ds(p * 64, 64)]

    def w_send(a, b, p, dev):
        send(w_piece(a, p), w_piece(b, p), w_sem.at[b * 4 + p], dev)

    def w_wait(k, p):
        arrived(w_piece(k, p), w_sem.at[k * 4 + p])
        if k == 3 and p % 2 == 0:
            w_send(3, 2, p, qp)
        if k == 1 and p % 2 == 1:
            w_send(1, 2, p, qm)

    def w_start():
        for p in range(4):
            w_send(0, 3, p, qp)
            w_send(0, 1, p, qm)

    def cols_of(h, n):
        return pl.ds(h * (npix // n), npix // n)

    def classes(k, part, h):
        n = CHUNKS[k]
        base = part * 64
        half = pl.ds(part * 128, 128)
        if k > 0 and h == 0:
            wn[k, half] = (wts[k, half].astype(F32) * scale[k, 0:1, :]).astype(BF16)
        for i in range(npix // n // 512):
            cols = pl.ds(h * (npix // n) + i * 512, 512)
            res = jnp.dot(wn[k, half], wgt[:, cols], preferred_element_type=F32)
            for g in range(4):
                cown[k, pl.ds(base + g * 16, 16), cols] = res[g * 32 : g * 32 + 16]
                cpart[k, pl.ds(base + g * 16, 16), cols] = res[g * 32 + 16 : g * 32 + 32].astype(BF16)
        at = (k, pl.ds(base, 64), cols_of(h, n))
        send(cpart.at[at], drecv.at[at], d_sem.at[(k * 2 + part) * MAXCH + h], pn)

    def own(k, j, dz, cols):
        return cown.at[k, pl.ds((PLACE[j] * 2 + dz) * 16, 16), cols]

    def ring_send(k, h, n, slot, value, dev):
        at = (k * 6 + slot, slice(None), cols_of(h, n))
        fsend[at] = value.astype(BF16)
        send(fsend.at[at], frecv.at[at], f_sem.at[(k * 6 + slot) * MAXCH + h], dev)

    def ring_wait(k, h, n, slot):
        at = (k * 6 + slot, slice(None), cols_of(h, n))
        arrived(frecv.at[at], f_sem.at[(k * 6 + slot) * MAXCH + h])
        return frecv[at].astype(F32)

    def first(k, part, h):
        n = CHUNKS[k]
        at = (k, pl.ds(part * 64, 64), cols_of(h, n))
        arrived(drecv.at[at], d_sem.at[(k * 2 + part) * MAXCH + h])

        def both(j, dz):
            there = drecv[k, pl.ds((PLACE[j] * 2 + dz) * 16, 16), cols_of(h, n)]
            return own(k, j, dz, cols_of(h, n))[...] + there.astype(F32)

        if part == 0:
            ring_send(k, h, n, 0, both(2, 0), fp)
            ring_send(k, h, n, 1, both(2, 1), fm)
            ring_send(k, h, n, 2, both(1, 1), fp)
            rest = ((1, 0),)
        else:
            ring_send(k, h, n, 3, both(3, 0), fm)
            rest = ((3, 1), (0, 0), (0, 1))
        for j, dz in rest:
            own(k, j, dz, cols_of(h, n))[...] = both(j, dz)

    def second(k, h, way):
        n = CHUNKS[k]
        j, dz, dev = ((1, 0, fp), (3, 1, fm))[way]
        value = own(k, j, dz, cols_of(h, n))[...] + ring_wait(k, h, n, way)
        ring_send(k, h, n, 4 + way, value, dev)

    late = []

    def s_wait(k, h):
        at = (k, slice(None) if k != 2 else 0, slice(None), cols_of(h, CHUNKS[k]))

        @pl.when(lax.rem(q + k, 4) != 0)
        def _():
            arrived(srecv.at[at], s_sem.at[k * MAXCH + h])

    def third(k, h):
        n = CHUNKS[k]
        cols = cols_of(h, n)
        parts = [ring_wait(k, h, n, slot) for slot in (2, 3, 4, 5)]
        one = (own(k, 0, 0, cols)[...] + parts[1] + parts[2]).astype(BF16)
        two = (own(k, 0, 1, cols)[...] + parts[0] + parts[3]).astype(BF16)
        s = lax.rem(q + k, 4)
        there = shifted(0, s)
        ssend[k, 0, :, cols] = one
        ssend[k, 1, :, cols] = two
        if k == 2:
            at = (slice(None), cols)
            send(ssend.at[(2, 1, *at)], szrecv.at[at], sz_sem.at[h], (there[0], 1 - z, *there[2:]))
        at = (k, slice(None) if k != 2 else 0, slice(None), cols)
        copy = pltpu.make_async_remote_copy(
            src_ref=ssend.at[at], dst_ref=srecv.at[at],
            send_sem=ss_sem.at[k * MAXCH + h], recv_sem=s_sem.at[k * MAXCH + h],
            device_id=there, device_id_type=MESH,
        )

        @pl.when(s != 0)
        def _():
            copy.start()

        @pl.when(s == 0)
        def _():
            srecv[k, 0, :, cols] = one
            if k != 2:
                srecv[k, 1, :, cols] = two

        late.append((s, copy))

    def zearly():
        for k in (0, 3, 1):
            for h in range(CHUNKS[k]):
                s_wait(k, h)
        for i in range(4):
            cols = cols_of(i, 4)
            mine, other = (
                sum(srecv[k, dz, :, cols].astype(F32) for k in (0, 3, 1)) for dz in (0, 1)
            )
            szown[:, cols] = mine
            zsend[:, cols] = other.astype(BF16)
        send(zsend, zrecv, z_sem, zn)

    def zwait():
        arrived(zrecv, z_sem)

    def final(h):
        cols = cols_of(h, CHUNKS[2])
        at = (slice(None), cols)
        s_wait(2, h)
        arrived(szrecv.at[at], sz_sem.at[h])
        out_ref[at] = (
            szown[at] + zrecv[at].astype(F32) + srecv[2, 0, :, cols].astype(F32) + szrecv[at].astype(F32)
        )

    prepare(3)
    ag(own_ref, 0, 1, 0, 0, sm)
    ag(own_ref, 3, 0, 0, 0, fp)
    prepare(1)
    got(1, 0, 0)
    to_second(1, 0)
    got(0, 1, 0)
    got(0, 0, 1)
    got(0, 3, 0)
    to_second(0, 1)
    prepare(2)
    ag(own_ref, 0, 0, 1, 0, pn)
    got(1, 3, 0)
    ag(slab(0, 0, 0, 1), 1, 0, 0, 1, fm)
    got(0, 2, 0)
    got(0, 1, 1)
    got(3, 0, 0)
    partners(0, 0)
    scores(0)
    rq_far(0)
    ag(slab(0, 0, 0, 1), 3, 0, 0, 1, fp)
    rq_near(0)
    to_second(3, 0)
    got(1, 1, 0)
    got(0, 3, 1)
    got(1, 0, 1)
    got(0, 2, 1)
    got(1, 2, 0)
    partners(0, 1)
    to_second(1, 1)
    scores(1)
    rq_far(1)
    partners(1, 0)
    scores(2)
    rq_far(2)
    got(2, 0, 0)
    rq_near(2)
    got(3, 3, 0)
    to_second(2, 0)
    rq_second(0, 0)
    got(2, 0, 1)
    got(1, 1, 1)
    to_second(2, 1)
    got(3, 1, 0)
    rq_second(0, 1)
    got(3, 2, 0)
    got(3, 0, 1)
    rq_near(1)
    rq_second(1, 1)
    rq_second(1, 0)
    rq_second(2, 1)
    got(1, 2, 1)
    to_second(3, 1)
    partners(3, 0)
    scores(6)
    got(2, 3, 0)
    rq_second(2, 0)
    got(2, 1, 1)
    got(2, 3, 1)
    got(1, 3, 1)
    rq_far(6)
    rq_near(6)
    partners(1, 1)
    got(2, 1, 0)
    scores(3)
    got(3, 3, 1)
    rq_far(3)
    got(3, 1, 1)
    rq_third(0)
    got(2, 2, 1)
    partners(2, 1)
    scores(5)
    got(2, 2, 0)
    rq_near(3)
    got(3, 2, 1)
    partners(3, 1)
    partners(2, 0)
    rq_far(5)
    scores(7)
    rq_second(6, 1)
    rq_far(7)
    rq_near(5)
    rq_second(6, 0)
    rq_second(5, 1)
    scores(4)
    rq_second(5, 0)
    rq_far(4)
    rq_third(1)
    rq_second(7, 1)
    rq_near(7)
    rq_third(6)
    rq_near(4)
    rq_second(4, 0)
    rq_third(2)
    rq_second(4, 1)
    rq_second(3, 1)
    rq_second(7, 0)
    rq_second(3, 0)
    rq_third(7)
    rq_third(5)
    rq_third(4)
    rq_third(3)
    peak()
    w_start()
    softmax()
    classes(0, 0, 0)
    classes(0, 1, 0)
    first(0, 0, 0)
    w_wait(3, 1)
    first(0, 1, 0)
    w_wait(1, 0)
    w_wait(1, 1)
    w_wait(3, 0)
    classes(3, 0, 0)
    classes(1, 0, 0)
    second(0, 0, 0)
    classes(1, 0, 1)
    w_wait(1, 2)
    second(0, 0, 1)
    first(3, 0, 0)
    first(1, 0, 0)
    w_wait(3, 3)
    w_wait(3, 2)
    classes(3, 1, 0)
    w_wait(1, 3)
    classes(1, 1, 0)
    first(1, 0, 1)
    classes(1, 1, 1)
    first(3, 1, 0)
    second(3, 0, 1)
    w_wait(2, 1)
    w_wait(2, 0)
    second(3, 0, 0)
    classes(2, 0, 0)
    classes(2, 0, 1)
    first(1, 1, 1)
    second(1, 1, 0)
    third(0, 0)
    second(1, 1, 1)
    second(1, 0, 0)
    first(2, 0, 0)
    first(1, 1, 0)
    w_wait(2, 3)
    w_wait(2, 2)
    classes(2, 1, 0)
    third(3, 0)
    second(1, 0, 1)
    third(1, 1)
    classes(2, 1, 1)
    first(2, 0, 1)
    second(2, 0, 0)
    first(2, 1, 0)
    second(2, 0, 1)
    third(1, 0)
    first(2, 1, 1)
    second(2, 1, 1)
    second(2, 1, 0)
    zearly()
    third(2, 0)
    third(2, 1)
    zwait()
    final(0)
    final(1)

    for s, copy in late:

        @pl.when(s != 0)
        def _():
            copy.wait_send()

    for copy in sends:
        copy.wait_send()


def body(particles, ctf, noise_var, projections, orient_class, class_prior, counts):
    npart, npix = particles.shape
    vmem = pl.BlockSpec(memory_space=pltpu.VMEM)
    smem = pl.BlockSpec(memory_space=pltpu.SMEM)
    hbm = pl.BlockSpec(memory_space=pl.ANY)
    dma = pltpu.SemaphoreType.DMA
    out, norm = pl.pallas_call(
        kernel,
        out_shape=(jax.ShapeDtypeStruct((16, npix), F32), jax.ShapeDtypeStruct((1, npart), F32)),
        in_specs=[hbm, hbm, hbm, hbm, hbm, smem, smem],
        out_specs=(vmem, vmem),
        scratch_shapes=[
            pltpu.VMEM((1, npix), F32),
            pltpu.VMEM((16, npix), BF16),
            pltpu.VMEM((1, 1024), jnp.int32),
            pltpu.VMEM((npart, npix), BF16),
            pltpu.VMEM((npart, npix), BF16),
            pltpu.VMEM((npix, npart), BF16),
            pltpu.VMEM((npix, npart), BF16),
            pltpu.VMEM((1024, npix), BF16),
            pltpu.VMEM((128, npix), BF16),
            pltpu.VMEM((1024, npart), F32),
            pltpu.VMEM((48, 16, npart), F32),
            pltpu.VMEM((256, npart), F32),
            pltpu.VMEM((4, 8, npart), F32),
            pltpu.VMEM((4, 256, npart), BF16),
            pltpu.VMEM((4, 128, npix), F32),
            pltpu.VMEM((4, 128, npix), BF16),
            pltpu.VMEM((4, 128, npix), BF16),
            pltpu.VMEM((24, 16, npix), BF16),
            pltpu.VMEM((24, 16, npix), BF16),
            pltpu.VMEM((4, 2, 16, npix), BF16),
            pltpu.VMEM((4, 2, 16, npix), BF16),
            pltpu.VMEM((16, npix), BF16),
            pltpu.VMEM((16, npix), F32),
            pltpu.VMEM((16, npix), BF16),
            pltpu.VMEM((16, npix), BF16),
            pltpu.VMEM((4, 256, npart), BF16),
            pltpu.VMEM((4, 8, npart), F32),
            dma((11,)), dma((NSEM,)), dma((64,)), dma((48,)), dma((4,)), dma((16,)), dma((8 * MAXCH,)),
            dma((24 * MAXCH,)), dma((4 * MAXCH,)), dma((4 * MAXCH,)), dma((MAXCH,)), dma,
        ],
        compiler_params=pltpu.CompilerParams(
            collective_id=0, has_side_effects=True, vmem_limit_bytes=64 * 1024 * 1024 - 128 * 1024
        ),
    )(particles, ctf, noise_var.reshape(1, npix), projections, orient_class.reshape(1, 1024), class_prior, counts)
    return out, norm.reshape(npart)


def solution(mesh):
    torus = Mesh(
        mesh.devices.reshape(4, 2, 4, 2, mesh.shape["pix"]),
        ("blk_0", "blk_1", "blk_2", "blk_3", "pix"),
    )
    in_specs = (P(BLK, "pix"), P(BLK, "pix"), P("pix"), P(BLK, "pix"), P(), P(), P(BLK))
    out_specs = (P(BLK, "pix"), P(BLK))
    return jax.shard_map(body, mesh=torus, in_specs=in_specs, out_specs=out_specs, check_vma=False)
```
